16 devices in a mesh: data: 16 (over z, y, x, core).
Axes of the slice: x: 2, y: 2, z: 2, core: 2. Of those that a mesh axis runs over, the one named last changes fastest.
Arguments:
- x_tokens: bfloat16 [8192, 1024], P('data')
- labels: int32 [3, 8192], P(None, 'data')
- w_up: bfloat16 [4, 1024, 4096], replicated
- w_down: bfloat16 [4, 4096, 1024], replicated
- task_heads: bfloat16 [3, 1024, 3], replicated
Outputs:
- output 1: float32 [3], replicated
- output 2: float32 [3, 3], replicated
- output 3: float32 [4, 4194304], P(None, 'data')
- output 4: float32 [4, 4194304], P(None, 'data')
All inputs are finite; a program needn't handle non-finite values.
Results may differ from the reference program's by a relative error of at most 0.01256.
Values are sent between devices in bfloat16 or wider.
A program may use at most 1 GiB of HBM per device.

```python
import jax
import jax.numpy as jnp
from jax import lax

D_MODEL = 1024
D_FF = 4096
NUM_TASKS = 3
NUM_CLASSES = 3
NUM_LAYERS = 4
TOK_DEV = 512
NUM_DEV = 16
EG_STEPS = 20


def setup_inputs(seed: int = 0) -> dict:
    base_key = jax.random.key(seed)
    sub_keys = jax.random.split(base_key, 10)
    num_tokens = NUM_DEV * TOK_DEV
    x_tokens = jax.random.normal(sub_keys[0], (num_tokens, D_MODEL), jnp.float32).astype(jnp.bfloat16)
    w_up = (jax.random.normal(sub_keys[1], (NUM_LAYERS, D_MODEL, D_FF), jnp.float32) * D_MODEL ** -0.5).astype(jnp.bfloat16)
    w_down = (jax.random.normal(sub_keys[2], (NUM_LAYERS, D_FF, D_MODEL), jnp.float32) * D_FF ** -0.5).astype(jnp.bfloat16)
    shared_head = jax.random.normal(sub_keys[3], (D_MODEL, NUM_CLASSES), jnp.float32)
    head_noise = jax.random.normal(sub_keys[4], (NUM_TASKS, D_MODEL, NUM_CLASSES), jnp.float32)
    task_order = jax.random.permutation(sub_keys[5], NUM_TASKS)
    task_sign = jnp.where(task_order < NUM_TASKS // 2, -1.0, 1.0)
    task_heads = ((task_sign[:, None, None] * shared_head[None] + 0.6 * head_noise) * D_MODEL ** -0.5).astype(jnp.bfloat16)
    dev_shift = jax.random.randint(sub_keys[6], (NUM_DEV, 1), 0, NUM_CLASSES)
    local_lab = jax.random.randint(sub_keys[7], (NUM_DEV, TOK_DEV), 0, max(NUM_CLASSES // 2, 1))
    base_lab = ((local_lab + dev_shift) % NUM_CLASSES).reshape(1, num_tokens)
    free_lab = jax.random.randint(sub_keys[8], (NUM_TASKS, num_tokens), 0, NUM_CLASSES)
    free_pick = jax.random.randint(sub_keys[9], (NUM_TASKS, num_tokens), 0, 4)
    labels = jnp.where(free_pick == 0, free_lab, base_lab).astype(jnp.int32)
    return {'x_tokens': x_tokens, 'labels': labels, 'w_up': w_up, 'w_down': w_down, 'task_heads': task_heads}


def simplex_weights(gram_mat):
    temperature = jnp.trace(gram_mat) / NUM_TASKS
    alpha_vec = jnp.full((NUM_TASKS,), 1.0 / NUM_TASKS, jnp.float32)
    for step_idx in range(EG_STEPS):
        grad_pull = jnp.sum(gram_mat * alpha_vec[None, :], axis=1)
        alpha_vec = alpha_vec * jnp.exp(-grad_pull / temperature)
        alpha_vec = alpha_vec / jnp.sum(alpha_vec)
    return alpha_vec


def block_grads(x_block, lab_block, w_up, w_down, task_heads):
    hidden = x_block
    saved_acts = []
    for layer_idx in range(NUM_LAYERS):
        pre_act = jnp.dot(hidden, w_up[layer_idx], preferred_element_type=jnp.float32)
        act_val, gelu_slope = jax.jvp(jax.nn.gelu, (pre_act,), (jnp.ones_like(pre_act),))
        act_bf = act_val.astype(jnp.bfloat16)
        mlp_out = jnp.dot(act_bf, w_down[layer_idx], preferred_element_type=jnp.float32)
        saved_acts.append((hidden, act_bf, gelu_slope))
        hidden = (hidden.astype(jnp.float32) + mlp_out).astype(jnp.bfloat16)
    heads_f = task_heads.astype(jnp.float32)
    logits = jnp.einsum('bd,tdc->tbc', hidden.astype(jnp.float32), heads_f)
    soft_probs = jax.nn.softmax(logits, axis=-1)
    onehot = (lab_block[:, :, None] == jnp.arange(NUM_CLASSES)[None, None, :]).astype(jnp.float32)
    head_err = (soft_probs - onehot).astype(jnp.bfloat16)
    d_hidden = jnp.einsum('tbc,tdc->tbd', head_err.astype(jnp.float32), heads_f).astype(jnp.bfloat16)
    up_list = []
    down_list = []
    for layer_idx in range(NUM_LAYERS - 1, -1, -1):
        hidden_in, act_bf, gelu_slope = saved_acts[layer_idx]
        d_hid_f = d_hidden.astype(jnp.float32)
        down_list.append(jnp.einsum('bf,tbd->tfd', act_bf.astype(jnp.float32), d_hid_f))
        d_act = jnp.einsum('tbd,fd->tbf', d_hid_f, w_down[layer_idx].astype(jnp.float32))
        d_pre = (d_act * gelu_slope[None]).astype(jnp.bfloat16)
        d_pre_f = d_pre.astype(jnp.float32)
        up_list.append(jnp.einsum('bd,tbf->tdf', hidden_in.astype(jnp.float32), d_pre_f))
        if layer_idx > 0:
            d_hidden = (d_hid_f + jnp.einsum('tbf,df->tbd', d_pre_f, w_up[layer_idx].astype(jnp.float32))).astype(jnp.bfloat16)
    return jnp.stack(up_list[::-1]), jnp.stack(down_list[::-1])


def reference(x_tokens, labels, w_up, w_down, task_heads):
    x_blocks = x_tokens.reshape(NUM_DEV, TOK_DEV, D_MODEL)
    lab_blocks = jnp.transpose(labels.reshape(NUM_TASKS, NUM_DEV, TOK_DEV), (1, 0, 2))
    zero_up = jnp.zeros((NUM_LAYERS, NUM_TASKS, D_MODEL, D_FF), jnp.float32)
    zero_down = jnp.zeros((NUM_LAYERS, NUM_TASKS, D_FF, D_MODEL), jnp.float32)

    def scan_body(running, token_block):
        up_grads, down_grads = block_grads(token_block[0], token_block[1], w_up, w_down, task_heads)
        return (running[0] + up_grads, running[1] + down_grads), None

    totals, unused = lax.scan(scan_body, (zero_up, zero_down), (x_blocks, lab_blocks))
    inv_tokens = 1.0 / (NUM_DEV * TOK_DEV)
    flat_up = (totals[0] * inv_tokens).reshape(NUM_LAYERS, NUM_TASKS, D_MODEL * D_FF)
    flat_down = (totals[1] * inv_tokens).reshape(NUM_LAYERS, NUM_TASKS, D_FF * D_MODEL)
    gram_mat = jnp.einsum('lts,lus->tu', flat_up, flat_up) + jnp.einsum('lts,lus->tu', flat_down, flat_down)
    task_weights = simplex_weights(gram_mat)
    grad_up = jnp.einsum('t,lts->ls', task_weights, flat_up)
    grad_down = jnp.einsum('t,lts->ls', task_weights, flat_down)
    return (task_weights, gram_mat, grad_up, grad_down)
```

```python
import jax
import jax.numpy as jnp
from jax import lax
from jax.sharding import PartitionSpec as P

EG_STEPS = 20
F32 = jnp.float32
BF16 = jnp.bfloat16


def simplex_weights(gram_mat):
    num_tasks = gram_mat.shape[0]
    tau = jnp.trace(gram_mat) / num_tasks
    alpha_vec = jnp.full((num_tasks,), 1.0 / num_tasks, F32)
    for step_idx in range(EG_STEPS):
        grad_pull = jnp.sum(gram_mat * alpha_vec[None, :], axis=1)
        alpha_vec = alpha_vec * jnp.exp(-grad_pull / tau)
        alpha_vec = alpha_vec / jnp.sum(alpha_vec)
    return alpha_vec


def gelu_pair(pre_act):
    act_val, slope = jax.jvp(jax.nn.gelu, (pre_act,), (jnp.ones_like(pre_act),))
    return act_val.astype(BF16), slope


def solution(mesh):
    num_dev = mesh.shape['data']

    def local_step(x_local, lab_local, w_up, w_down, task_heads):
        num_layers, d_model, d_ff = w_up.shape
        num_tasks, _, num_classes = task_heads.shape
        num_tok = x_local.shape[0] * num_dev
        inv_tokens = 1.0 / num_tok
        me = lax.axis_index('data')
        width = d_ff // num_dev

        hidden = x_local
        slopes = []
        hidden_all = []
        for layer_idx in range(num_layers):
            hidden_all.append(lax.all_gather(hidden, 'data', axis=0, tiled=True))
            pre_act = jnp.dot(hidden, w_up[layer_idx], preferred_element_type=F32)
            act_bf, slope = gelu_pair(pre_act)
            mlp_out = jnp.dot(act_bf, w_down[layer_idx], preferred_element_type=F32)
            slopes.append(slope)
            hidden = (hidden.astype(F32) + mlp_out).astype(BF16)
        logits = jnp.einsum('bd,tdc->tbc', hidden, task_heads, preferred_element_type=F32)
        soft_probs = jax.nn.softmax(logits, axis=-1)
        onehot = (lab_local[:, :, None] == jnp.arange(num_classes)[None, None, :]).astype(F32)
        head_err = (soft_probs - onehot).astype(BF16)
        err_all = lax.all_gather(head_err, 'data', axis=1, tiled=True)

        def top_delta(err):
            return jnp.einsum('tbc,tdc->tbd', err, task_heads, preferred_element_type=F32).astype(BF16)

        delta_all = [None] * num_layers
        delta_all[num_layers - 1] = top_delta(err_all)
        delta = top_delta(head_err)
        for layer_idx in range(num_layers - 1, 0, -1):
            d_act = jnp.einsum('tbd,fd->tbf', delta, w_down[layer_idx], preferred_element_type=F32)
            d_pre = (d_act * slopes[layer_idx][None]).astype(BF16)
            delta = (delta.astype(F32) + jnp.einsum('tbf,df->tbd', d_pre, w_up[layer_idx], preferred_element_type=F32)).astype(BF16)
            delta_all[layer_idx - 1] = lax.all_gather(delta, 'data', axis=1, tiled=True)

        ups = [None] * num_layers
        downs = [None] * num_layers
        for layer_idx in range(num_layers - 1, -1, -1):
            wu = lax.dynamic_slice_in_dim(w_up[layer_idx], me * width, width, 1)
            wd = lax.dynamic_slice_in_dim(w_down[layer_idx], me * width, width, 0)
            h_in = hidden_all[layer_idx]
            d_in = delta_all[layer_idx]
            act_bf, slope = gelu_pair(jnp.dot(h_in, wu, preferred_element_type=F32))
            downs[layer_idx] = [jnp.einsum('bf,bd->fd', act_bf, d_in[t], preferred_element_type=F32) * inv_tokens for t in range(num_tasks)]
            ups[layer_idx] = []
            for t in range(num_tasks):
                d_act = jnp.einsum('bd,fd->bf', d_in[t], wd, preferred_element_type=F32)
                d_pre = (d_act * slope).astype(BF16)
                ups[layer_idx].append(jnp.einsum('bd,bf->df', h_in, d_pre, preferred_element_type=F32) * inv_tokens)

        pairs = [(t, s) for t in range(num_tasks) for s in range(t, num_tasks)]
        parts = [sum(jnp.sum(g[t] * g[s]) for g in ups + downs) for t, s in pairs]
        sums = lax.psum(jnp.stack(parts), 'data')
        rows = [[sums[pairs.index((min(t, s), max(t, s)))] for s in range(num_tasks)] for t in range(num_tasks)]
        gram_mat = jnp.stack([jnp.stack(r) for r in rows])
        alpha = simplex_weights(gram_mat)
        mix = lambda g: sum(alpha[t] * g[t] for t in range(num_tasks))
        grad_down = jnp.stack([mix(g).reshape(-1) for g in downs])
        g_up = jnp.stack([mix(g) for g in ups])
        g_up = lax.all_to_all(g_up, 'data', 1, 2, tiled=True)
        return alpha, gram_mat, g_up.reshape(num_layers, -1), grad_down

    return jax.shard_map(local_step, mesh=mesh, in_specs=(P('data', None), P(None, 'data'), P(), P(), P()), out_specs=(P(), P(), P(None, 'data'), P(None, 'data')), check_vma=False)
```
